16 devices in a mesh: rep: 1, dp: 16 (over x, y, z, core).
Axes of the slice: x: 2, y: 2, z: 2, core: 2. Of those that a mesh axis runs over, the one named last changes fastest.
Arguments:
- x: bfloat16 [16, 2048, 1024], P(('rep', 'dp'))
- dy: bfloat16 [16, 2048, 1024], P(('rep', 'dp'))
- wq: bfloat16 [2, 1024, 1024], P(None, 'dp')
- wk: bfloat16 [2, 1024, 1024], P(None, 'dp')
- wv: bfloat16 [2, 1024, 1024], P(None, 'dp')
- wo: bfloat16 [2, 1024, 1024], P(None, 'dp')
- w_gate: bfloat16 [2, 1024, 4096], P(None, 'dp')
- w_up: bfloat16 [2, 1024, 4096], P(None, 'dp')
- w_down: bfloat16 [2, 4096, 1024], P(None, 'dp')
Outputs:
- output 1: bfloat16 [16, 2048, 1024], P(('rep', 'dp'))
- output 2: bfloat16 [2, 1024, 1024], P('rep', 'dp')
- output 3: bfloat16 [2, 1024, 1024], P('rep', 'dp')
- output 4: bfloat16 [2, 1024, 1024], P('rep', 'dp')
- output 5: bfloat16 [2, 1024, 1024], P('rep', 'dp')
- output 6: bfloat16 [2, 1024, 4096], P('rep', 'dp')
- output 7: bfloat16 [2, 1024, 4096], P('rep', 'dp')
- output 8: bfloat16 [2, 4096, 1024], P('rep', 'dp')
All inputs are finite; a program needn't handle non-finite values.
Results may differ from the reference program's by a relative error of at most 0.0319.
Values are sent between devices in bfloat16 or wider.
A program may use at most 2 GiB of HBM per device.

```python
import jax
import jax.numpy as jnp
from jax import lax

SEQUENCES = 16
TOKENS = 2048
D = 1024
HEADS = 8
KV_HEADS = 8
HEAD = 128
FF = 4096
LAYERS = 2
THETA = 10000
NAMES = ("wq", "wk", "wv", "wo", "w_gate", "w_up", "w_down")
SHAPES = {
    "wq": (LAYERS, D, HEADS * HEAD),
    "wk": (LAYERS, D, KV_HEADS * HEAD),
    "wv": (LAYERS, D, KV_HEADS * HEAD),
    "wo": (LAYERS, HEADS * HEAD, D),
    "w_gate": (LAYERS, D, FF),
    "w_up": (LAYERS, D, FF),
    "w_down": (LAYERS, FF, D),
}


def bump(key, n, height):
    away = (jnp.arange(n, dtype=jnp.int32) - jax.random.randint(key, (), 0, n, jnp.int32)) % n
    return jnp.where(away < n // 8, height, 1.0)


def together(key, own, strength):
    shared = jax.random.normal(key, own.shape[1:], jnp.float32)
    return (own + strength * shared) * lax.rsqrt(1 + strength * strength)


def setup_inputs(seed: int = 0, part: int = 0) -> dict:
    kx, kdy, ka, kb, kz, kf, kh, kl, *keys = jax.random.split(jax.random.key(seed), 8 + 3 * len(NAMES))
    kx, kdy, ka, kb = (jax.random.fold_in(k, part) for k in (kx, kdy, ka, kb))
    kw, km, kv = (keys[i::3] for i in range(3))
    shape = (SEQUENCES, TOKENS, D)
    much_x, much_dy = jax.random.uniform(kz, (2,), jnp.float32, 0.0, 1.0)
    loud = 2.0 ** jax.random.uniform(jax.random.fold_in(kz, 1), (), jnp.float32, -1.0, 2.0)
    layers = 2.0 ** jax.random.uniform(kl, (LAYERS, 1, 1), jnp.float32, -1.0, 1.0)
    times = {"wq": 1.0, "wk": 1.0, "wv": 2.0, "wo": layers, "w_gate": 1.0, "w_up": bump(kh, FF, 4.0), "w_down": layers}
    x = together(ka, jax.random.normal(kx, shape, jnp.float32), much_x) * bump(kf, D, 4.0)
    dy = together(kb, jax.random.normal(kdy, shape, jnp.float32), much_dy)
    drawn = {"x": x.astype(jnp.bfloat16), "dy": (loud * dy * (SEQUENCES * TOKENS) ** -0.5).astype(jnp.bfloat16)}
    for key, name in zip(kw, NAMES, strict=True):
        drawn[name] = (jax.random.normal(key, SHAPES[name], jnp.float32) * SHAPES[name][1] ** -0.5 * times[name]).astype(jnp.bfloat16)
    return drawn


def matmul(a, w):
    return jnp.dot(a, w, preferred_element_type=jnp.float32).astype(jnp.bfloat16)


def normed(h):
    wide = h.astype(jnp.float32)
    scale = lax.rsqrt(jnp.mean(wide**2, -1, keepdims=True) + 1e-6)
    return (wide * scale).astype(jnp.bfloat16)


def turned(t, theta):
    half = t.shape[-1] // 2
    angle = jnp.arange(t.shape[0], dtype=jnp.float32)[:, None] * theta ** (-jnp.arange(half, dtype=jnp.float32) / half)
    cos, sin = jnp.cos(angle)[:, None], jnp.sin(angle)[:, None]
    a, b = t[..., :half].astype(jnp.float32), t[..., half:].astype(jnp.float32)
    return jnp.concatenate([a * cos - b * sin, b * cos + a * sin], -1).astype(jnp.bfloat16)


def seen_by(q, k, v):
    tokens, kv = q.shape[0], k.shape[1]
    q = q.reshape(tokens, kv, -1, q.shape[-1])
    scores = jnp.einsum("tgsd,ugd->gstu", q.astype(jnp.float32), k.astype(jnp.float32)) * q.shape[-1] ** -0.5
    place = jnp.arange(tokens)
    weights = jax.nn.softmax(jnp.where(place[:, None] >= place, scores, -jnp.inf), -1).astype(jnp.bfloat16)
    return jnp.einsum("gstu,ugd->tgsd", weights.astype(jnp.float32), v.astype(jnp.float32)).astype(jnp.bfloat16).reshape(tokens, -1)


def layer(h, w):
    a = normed(h)
    q, k = (turned(matmul(a, w[name]).reshape(h.shape[0], -1, HEAD), THETA) for name in ("wq", "wk"))
    h = h + matmul(seen_by(q, k, matmul(a, w["wv"]).reshape(h.shape[0], -1, HEAD)), w["wo"])
    b = normed(h)
    gate = jnp.dot(b, w["w_gate"], preferred_element_type=jnp.float32)
    up = jnp.dot(b, w["w_up"], preferred_element_type=jnp.float32)
    return h + matmul((jax.nn.silu(gate) * up).astype(jnp.bfloat16), w["w_down"])


def stack(weights, h):
    return lax.scan(lambda h, w: (layer(h, w), None), h, weights)[0]


def reference(x, dy, wq, wk, wv, wo, w_gate, w_up, w_down):
    weights = dict(zip(NAMES, (wq, wk, wv, wo, w_gate, w_up, w_down), strict=True))

    def take(so_far, sequence):
        h, by_y = sequence
        _, back = jax.vjp(stack, weights, h)
        by_weights, by_h = back(by_y)
        return jax.tree.map(lambda total, term: total + term.astype(jnp.float32), so_far, by_weights), by_h

    none_yet = {name: jnp.zeros(w.shape, jnp.float32) for name, w in weights.items()}
    by_weights, by_x = lax.scan(take, none_yet, (x, dy))
    return (by_x, *(by_weights[name].astype(jnp.bfloat16) for name in NAMES))
```

```python
import functools

import jax
import jax.numpy as jnp
from jax import lax
from jax.experimental import pallas as pl
from jax.experimental.pallas import tpu as pltpu
from jax.sharding import PartitionSpec as P

HEAD = 128
THETA = 10000
NEG = -1e30
HIDDEN = 2 * NEG
LOG2E = 1.4426950408889634
VMEM = 60 * 2**20
TILE = 1024
BF16, F32 = jnp.bfloat16, jnp.float32


def _dot(a, b, ca, cb):
    return lax.dot_general(a, b, (((ca,), (cb,)), ((), ())), preferred_element_type=F32)


def _call(kernel, grid, ins, outs, args, name, scratch=(), aliases=None, flops=0, moved=0):
    specs, shapes = zip(*outs)
    return pl.pallas_call(
        kernel,
        grid=grid,
        in_specs=list(ins),
        out_specs=list(specs),
        out_shape=list(shapes),
        scratch_shapes=list(scratch),
        input_output_aliases=aliases or {},
        compiler_params=pltpu.CompilerParams(dimension_semantics=("arbitrary",) * len(grid), vmem_limit_bytes=VMEM),
        cost_estimate=pl.CostEstimate(flops=int(flops), bytes_accessed=int(moved), transcendentals=0),
        name=name,
    )(*args)


def _like(shape, dtype=BF16):
    return jax.ShapeDtypeStruct(shape, dtype)


def _rows(tile, cols):
    return pl.BlockSpec((tile, cols), lambda m: (m, 0))


def _whole(shape):
    return pl.BlockSpec(shape, lambda *_: (0,) * len(shape), pipeline_mode=pl.Buffered(1))


def _scale(wide):
    return lax.rsqrt(jnp.mean(wide * wide, -1, keepdims=True) + 1e-6)


def _normed(h):
    wide = h.astype(F32)
    return (wide * _scale(wide)).astype(BF16)


def _norm_back(h, g):
    wide, g = h.astype(F32), g.astype(F32)
    r = _scale(wide)
    return (g * r - wide * (r * r * r * jnp.mean(g * wide, -1, keepdims=True))).astype(BF16)


def _plus(a, b):
    return (a.astype(F32) + b.astype(F32)).astype(BF16)


def _qkv_kernel(h_ref, w_ref, cos_ref, sin_ref, a_ref, q_ref, k_ref, v_ref):
    a = _normed(h_ref[...])
    a_ref[...] = a
    d = a.shape[1]
    for n, out in enumerate((q_ref, k_ref, v_ref)):
        t = _dot(a, w_ref[:, n * d : (n + 1) * d], 1, 0).astype(BF16)
        if n == 2:
            out[...] = t
            continue
        for at in range(0, d, HEAD):
            one = t[:, at : at + HEAD].astype(F32)
            out[:, at : at + HEAD] = (one * cos_ref[...] + pltpu.roll(one, HEAD // 2, 1) * sin_ref[...]).astype(BF16)


def qkv(h, w, cos, sin, tile=512):
    t, d = h.shape
    one = (_rows(tile, d), _like((t, d)))
    return _call(_qkv_kernel, (t // tile,), [_rows(tile, d), _whole((d, 3 * d)), _rows(tile, HEAD), _rows(tile, HEAD)], [one] * 4, (h, w, cos, sin), "qkv",
                 flops=2 * t * d * 3 * d, moved=16 * t * d)


def _out_kernel(o_ref, h_ref, w_ref, h2_ref, b_ref):
    h2 = _plus(h_ref[...], _dot(o_ref[...], w_ref[...], 1, 0).astype(BF16))
    h2_ref[...] = h2
    b_ref[...] = _normed(h2)


def attn_out(o, h, w, tile=512):
    t, d = h.shape
    array, at = w
    spec = pl.BlockSpec((d, d), lambda m: (0, at), pipeline_mode=pl.Buffered(1))
    one = (_rows(tile, d), _like((t, d)))
    return _call(_out_kernel, (t // tile,), [_rows(tile, d), _rows(tile, d), spec], [one] * 2, (o, h, array), "attn_out", flops=2 * t * d * d, moved=8 * t * d)


def _gate_up_kernel(b_ref, wg_ref, wu_ref, gu_ref, p_ref):
    b = b_ref[...]
    d = b.shape[1]
    wg, wu = wg_ref[...].reshape(d, -1), wu_ref[...].reshape(d, -1)
    n = wg.shape[1]
    for at in range(0, n, 256):
        cut = slice(at, at + 256)
        g, u = _dot(b, wg[:, cut], 1, 0), _dot(b, wu[:, cut], 1, 0)
        gu_ref[0, :, cut] = g
        gu_ref[1, :, cut] = u
        p_ref[:, cut] = (g * (1 / (1 + jnp.exp(-g))) * u).astype(BF16)


def gate_up(b, wg, wu, tile=512):
    t, d = b.shape
    ff = 4 * TILE
    return _call(_gate_up_kernel, (ff // TILE, t // tile),
                 [pl.BlockSpec((tile, d), lambda n, m: (m, 0)), wg[1](lambda n, m: n), wu[1](lambda n, m: n)],
                 [(pl.BlockSpec((2, tile, TILE), lambda n, m: (0, m, n)), _like((2, t, ff), F32)), (pl.BlockSpec((tile, TILE), lambda n, m: (m, n)), _like((t, ff)))],
                 (b, wg[0], wu[0]), "gate_up", flops=4 * t * d * ff, moved=10 * t * ff)


def _down_kernel(p_ref, w_ref, h_ref, out_ref, acc):
    k = pl.program_id(1)

    @pl.when(k == 0)
    def _():
        acc[...] = jnp.zeros_like(acc)

    acc[...] += _dot(p_ref[...], w_ref[...].reshape(p_ref.shape[1], -1), 1, 0)

    @pl.when(k == pl.num_programs(1) - 1)
    def _():
        out_ref[...] = _plus(h_ref[...], acc[...].astype(BF16))


def down(p, h, wd, tile=1024):
    t, d = h.shape
    ff = p.shape[1]
    row = pl.BlockSpec((tile, d), lambda m, k: (m, 0))
    return _call(_down_kernel, (t // tile, ff // TILE), [pl.BlockSpec((tile, TILE), lambda m, k: (m, k)), wd[1](lambda m, k: k), row],
                 [(row, _like((t, d)))], (p, wd[0], h), "down", scratch=[pltpu.VMEM((tile, d), F32)], flops=2 * t * d * ff, moved=2 * t * ff)[0]


def _swish_back(g, u, dp):
    s = 1 / (1 + jnp.exp(-g))
    silu = g * s
    return silu, (dp * u * (s + silu * (1 - s))).astype(BF16), (dp * silu).astype(BF16)


def _ffn_last_kernel(b_ref, dy_ref, wg_ref, wu_ref, wd_ref, p_ref, dgu_ref):
    b, dy = b_ref[...], dy_ref[...]
    d = b.shape[1]
    wg, wu, wd = wg_ref[...].reshape(d, -1), wu_ref[...].reshape(d, -1), wd_ref[...].reshape(-1, d)
    for at in range(0, wg.shape[1], 256):
        cut = slice(at, at + 256)
        g, u = _dot(b, wg[:, cut], 1, 0), _dot(b, wu[:, cut], 1, 0)
        dp = _dot(dy, wd[cut, :], 1, 1).astype(BF16).astype(F32)
        silu, dg, du = _swish_back(g, u, dp)
        p_ref[:, cut] = (silu * u).astype(BF16)
        dgu_ref[0, :, cut] = dg
        dgu_ref[1, :, cut] = du


def ffn_last(b, dy, wg, wu, wd, tile=512):
    t, d = b.shape
    ff = 4 * TILE
    row = pl.BlockSpec((tile, d), lambda n, m: (m, 0))
    number = lambda n, m: n
    return _call(_ffn_last_kernel, (ff // TILE, t // tile), [row, row, wg[1](number), wu[1](number), wd[1](number)],
                 [(pl.BlockSpec((tile, TILE), lambda n, m: (m, n)), _like((t, ff))), (pl.BlockSpec((2, tile, TILE), lambda n, m: (0, m, n)), _like((2, t, ff)))],
                 (b, dy, wg[0], wu[0], wd[0]), "ffn_last", flops=6 * t * d * ff, moved=6 * t * ff)


def _ffn_back_kernel(dy_ref, wd_ref, gu_ref, dgu_ref):
    dy = dy_ref[...]
    wd = wd_ref[...].reshape(-1, dy.shape[1])
    for at in range(0, wd.shape[0], 256):
        cut = slice(at, at + 256)
        dp = _dot(dy, wd[cut, :], 1, 1).astype(BF16).astype(F32)
        _, dg, du = _swish_back(gu_ref[0, :, cut], gu_ref[1, :, cut], dp)
        dgu_ref[0, :, cut] = dg
        dgu_ref[1, :, cut] = du


def ffn_back(dy, wd, gu, tile=512):
    t, d = dy.shape
    ff = gu.shape[2]
    both = pl.BlockSpec((2, tile, TILE), lambda n, m: (0, m, n))
    return _call(_ffn_back_kernel, (ff // TILE, t // tile), [pl.BlockSpec((tile, d), lambda n, m: (m, 0)), wd[1](lambda n, m: n), both],
                 [(both, _like((2, t, ff)))], (dy, wd[0], gu), "ffn_back", flops=2 * t * d * ff, moved=12 * t * ff)[0]


def _ffn_in_kernel(dgu_ref, wg_ref, wu_ref, h_ref, dy_ref, out_ref, acc):
    k = pl.program_id(1)
    d = out_ref.shape[1]

    @pl.when(k == 0)
    def _():
        acc[...] = jnp.zeros_like(acc)

    acc[...] += _dot(dgu_ref[0], wg_ref[...].reshape(d, -1), 1, 1) + _dot(dgu_ref[1], wu_ref[...].reshape(d, -1), 1, 1)

    @pl.when(k == pl.num_programs(1) - 1)
    def _():
        out_ref[...] = _plus(dy_ref[...], _norm_back(h_ref[...], acc[...].astype(BF16)))


def ffn_in(dgu, wg, wu, h, dy, tile=1024):
    t, d = h.shape
    ff = dgu.shape[2]
    row = pl.BlockSpec((tile, d), lambda m, k: (m, 0))
    number = lambda m, k: k
    return _call(_ffn_in_kernel, (t // tile, ff // TILE), [pl.BlockSpec((2, tile, TILE), lambda m, k: (0, m, k)), wg[1](number), wu[1](number), row, row],
                 [(row, _like((t, d)))], (dgu, wg[0], wu[0], h, dy), "ffn_in", scratch=[pltpu.VMEM((tile, d), F32)], flops=4 * t * d * ff, moved=4 * t * ff)[0]


def _grad_kernel(a_ref, b_ref, *rest):
    out = rest[-1]
    out[...] = _dot(a_ref[...].reshape(a_ref.shape[-2:]), b_ref[...].reshape(b_ref.shape[-2:]), 0, 0).astype(BF16).reshape(out.shape)


def ffn_grads(p, dy, b, dgu):
    t, d = dy.shape
    ff = p.shape[1]
    shape = _like((16, 4, ff // 64, 3 * TILE))
    part = ff // TILE
    got = _call(_grad_kernel, (part,), [pl.BlockSpec((t, TILE), lambda j: (0, j)), _whole((t, d))],
                [(pl.BlockSpec((16 // part, 4, ff // 64, TILE), lambda j: (j, 0, 0, 0)), shape)], (p, dy), "grad_down", flops=2 * t * d * ff, moved=2 * t * ff)[0]
    return _call(_grad_kernel, (2, part), [_whole((t, d)), pl.BlockSpec((1, t, TILE), lambda i, j: (i, 0, j)), pl.BlockSpec(memory_space=pl.ANY)],
                 [(pl.BlockSpec((16, 1, ff // 64, TILE), lambda i, j: (0, j, 0, 1 + i)), shape)], (b, dgu, got), "grad_gate_up", aliases={2: 0},
                 flops=4 * t * d * ff, moved=4 * t * ff)[0]


def _out_back_kernel(dh_ref, w_ref, o_ref, do_ref, delta_ref):
    do = _dot(dh_ref[...], w_ref[...], 1, 1).astype(BF16)
    do_ref[...] = do
    both = do.astype(F32) * o_ref[...].astype(F32)
    for n in range(delta_ref.shape[0]):
        delta_ref[n : n + 1, :] = both[:, n * HEAD : (n + 1) * HEAD].T.sum(axis=0, keepdims=True)


def out_back(dh, w, o, tile=512):
    t, d = dh.shape
    array, at = w
    spec = pl.BlockSpec((d, d), lambda m: (0, at), pipeline_mode=pl.Buffered(1))
    return _call(_out_back_kernel, (t // tile,), [_rows(tile, d), spec, _rows(tile, d)],
                 [(_rows(tile, d), _like((t, d))), (pl.BlockSpec((d // HEAD, tile), lambda m: (0, m)), _like((d // HEAD, t), F32))],
                 (dh, array, o), "out_back", flops=2 * t * d * d, moved=8 * t * d)


def _qkv_back_kernel(dq_ref, dk_ref, dv_ref, w_ref, h_ref, dh_ref, out_ref):
    d = h_ref.shape[1]
    parts = [_dot(x[...], w_ref[:, n * d : (n + 1) * d], 1, 1) for n, x in enumerate((dq_ref, dk_ref, dv_ref))]
    out_ref[...] = _plus(dh_ref[...], _norm_back(h_ref[...], (parts[0] + parts[1] + parts[2]).astype(BF16)))


def qkv_back(dq, dk, dv, w, h, dh, tile=512):
    t, d = h.shape
    row = _rows(tile, d)
    spec = pl.BlockSpec((d, 3 * d), lambda m: (0, 0), pipeline_mode=pl.Buffered(1))
    return _call(_qkv_back_kernel, (t // tile,), [row] * 3 + [spec, row, row], [(row, _like((t, d)))], (dq, dk, dv, w, h, dh), "qkv_back",
                 flops=6 * t * d * d, moved=12 * t * d)[0]


def _attn_grads_kernel(a_ref, dq_ref, dk_ref, dv_ref, o_ref, dh_ref, out_ref, acc):
    i, k = pl.program_id(0), pl.program_id(1)

    @pl.when(k == 0)
    def _():
        acc[...] = jnp.zeros_like(acc)

    for n, (left, right) in enumerate(((o_ref, dh_ref), (a_ref, dq_ref), (a_ref, dk_ref), (a_ref, dv_ref))):

        @pl.when(i == n)
        def _():
            acc[...] += _dot(left[...], right[...], 0, 0)

    @pl.when(k == pl.num_programs(1) - 1)
    def _():
        out_ref[...] = acc[...].astype(BF16)


def attn_grads(a, dq, dk, dv, o, dh, tile=512):
    t, d = a.shape
    last = t // tile - 1

    def when(n):
        return pl.BlockSpec((tile, d), lambda i, k: (jnp.where(i == n, k, jnp.where(i < n, 0, last)), 0))

    return _call(_attn_grads_kernel, (4, t // tile), [pl.BlockSpec((tile, d), lambda i, k: (jnp.where(i == 0, 0, k), 0)), when(1), when(2), when(3), when(0), when(0)],
                 [(pl.BlockSpec((d, d), lambda i, k: (0, i)), _like((d, 4 * d + d // 2)))], (a, dq, dk, dv, o, dh), "attn_grads",
                 scratch=[pltpu.VMEM((d, d), F32)], flops=8 * t * d * d, moved=20 * t * d)[0]


def _mask(bk, wide, at):
    return lax.broadcasted_iota(jnp.int32, (bk, wide), 1) + at >= lax.broadcasted_iota(jnp.int32, (bk, wide), 0)


def _attend_kernel(q_ref, k_ref, v_ref, o_ref, lse_ref, top_s, mix_s, *, bq, bk):
    kb = q_ref.shape[1] // HEAD
    iq = pl.program_id(1)
    scale = HEAD**-0.5
    e = scale * LOG2E
    ones = jnp.ones((8, bk), BF16)
    top_s[...] = jnp.full_like(top_s, NEG)
    mix_s[...] = jnp.zeros_like(mix_s)

    def block(j, masked):
        here = pl.ds(j * bk, bk)
        heads = [slice(i * HEAD, (i + 1) * HEAD) for i in range(kb)]
        scores = [_dot(k_ref[here, at], q_ref[:, at], 1, 1) for at in heads]
        ok = _mask(bk, bq, 0) if masked else None
        weights, keeps = [], []
        for i, s in enumerate(scores):
            if masked:
                s = jnp.where(ok, s, HIDDEN)
            old = top_s[i : i + 1, :]
            top = jnp.maximum(old, s.max(axis=0, keepdims=True))
            top_s[i : i + 1, :] = top
            weights.append(jnp.exp2((s - top) * e).astype(BF16))
            keeps.append(jnp.exp2((old - top) * e))
        for i, (p, keep) in enumerate(zip(weights, keeps)):
            values = jnp.concatenate([v_ref[here, heads[i]].T, ones], axis=0)
            mix_s[i] = mix_s[i] * keep + _dot(values, p, 1, 0)

    lax.fori_loop(0, iq, lambda j, _: block(j, False), None)
    block(iq, True)
    for i in range(kb):
        top, total = top_s[i : i + 1, :], mix_s[i, HEAD : HEAD + 1, :]
        o_ref[:, i * HEAD : (i + 1) * HEAD] = (mix_s[i, :HEAD, :] * (1 / total)).T.astype(BF16)
        lse_ref[i : i + 1, :] = top * scale + jnp.log(total)


def attend(q, k, v, bq=512):
    t, d = q.shape
    kb = d // HEAD
    row = pl.BlockSpec((bq, d), lambda ih, iq: (iq, ih))
    keys = pl.BlockSpec((t, d), lambda ih, iq: (0, ih))
    return _call(functools.partial(_attend_kernel, bq=bq, bk=bq), (1, t // bq), [row, keys, keys],
                 [(row, _like((t, d))), (pl.BlockSpec((kb, bq), lambda ih, iq: (ih, iq)), _like((kb, t), F32))], (q, k, v), "attend",
                 scratch=[pltpu.VMEM((kb, bq), F32), pltpu.VMEM((kb, HEAD + 8, bq), F32)], flops=4 * t * t * d, moved=8 * t * d)


def _attend_back_kernel(q_ref, k_ref, v_ref, do_ref, lse_ref, delta_ref, cos_ref, sin_ref, dq_ref, dk_ref, dv_ref, dq_s, dk_s, dv_s, *, bq, bk):
    kb = q_ref.shape[1] // HEAD
    iq = pl.program_id(1)
    scale = HEAD**-0.5
    e = scale * LOG2E
    heads = [slice(i * HEAD, (i + 1) * HEAD) for i in range(kb)]

    @pl.when(iq == 0)
    def _():
        dk_s[...] = jnp.zeros_like(dk_s)
        dv_s[...] = jnp.zeros_like(dv_s)

    dq_s[...] = jnp.zeros_like(dq_s)
    lses = [lse_ref[0, i : i + 1, :] * LOG2E for i in range(kb)]
    deltas = [delta_ref[0, i : i + 1, :] for i in range(kb)]

    def block(j, masked):
        here = pl.ds(j * bk, bk)
        scores = [_dot(k_ref[here, at], q_ref[:, at], 1, 1) for at in heads]
        dps = [_dot(v_ref[here, at], do_ref[:, at], 1, 1) for at in heads]
        ok = _mask(bk, bq, 0) if masked else None
        for i, at in enumerate(heads):
            p = jnp.exp2(scores[i] * e - lses[i])
            if masked:
                p = jnp.where(ok, p, 0.0)
            ds = (p * (dps[i] - deltas[i])).astype(BF16)
            dv_s[here, at] += _dot(p.astype(BF16), do_ref[:, at], 1, 0)
            dk_s[here, at] += _dot(ds, q_ref[:, at], 1, 0)
            dq_s[i] += _dot(k_ref[here, at].T, ds, 1, 0)

    def turned_back(g, cos, sin):
        g = g.astype(BF16).astype(F32)
        return (g * cos + pltpu.roll(g * sin, HEAD // 2, 1)).astype(BF16)

    lax.fori_loop(0, iq, lambda j, _: block(j, False), None)
    block(iq, True)
    rows = pl.ds(iq * bq, bq)
    for i, at in enumerate(heads):
        dq_ref[:, at] = turned_back((dq_s[i] * scale).T, cos_ref[rows, :], sin_ref[rows, :])

    @pl.when(iq == pl.num_programs(1) - 1)
    def _():
        for at in heads:
            dk_ref[:, at] = turned_back(dk_s[:, at] * scale, cos_ref[...], sin_ref[...])
        dv_ref[...] = dv_s[...].astype(BF16)


def attend_back(q, k, v, do, lse, delta, cos, sin, bq=512, kb=4):
    t, d = q.shape
    w = kb * HEAD
    row = pl.BlockSpec((bq, w), lambda ih, iq: (iq, ih))
    keys = pl.BlockSpec((t, w), lambda ih, iq: (0, ih))
    stats = pl.BlockSpec((1, kb, bq), lambda ih, iq: (ih, 0, iq))
    one = _like((t, d))
    cut = lambda s: s.reshape(d // w, kb, t)
    return _call(functools.partial(_attend_back_kernel, bq=bq, bk=bq), (d // w, t // bq), [row, keys, keys, row, stats, stats, _whole(cos.shape), _whole(sin.shape)],
                 [(row, one), (keys, one), (keys, one)], (q, k, v, do, cut(lse), cut(delta), cos, sin), "attend_back",
                 scratch=[pltpu.VMEM((kb, HEAD, bq), F32), pltpu.VMEM((t, w), F32), pltpu.VMEM((t, w), F32)], flops=10 * t * t * d, moved=14 * t * d)


def _columns(array, first):
    return array, lambda number: pl.BlockSpec((array.shape[0], TILE), lambda *ids: (0, first + number(*ids)))


def _split(array, at):
    view = array.reshape(16, 4, 64, 3 * TILE)
    return view, lambda number: pl.BlockSpec((16, 1, 64, TILE), lambda *ids: (0, number(*ids), 0, at))


def _down_of(array):
    return array, lambda number: pl.BlockSpec((TILE, TILE), lambda *ids: (number(*ids), 0))


def rotary(t):
    half = HEAD // 2
    angle = jnp.arange(t, dtype=F32)[:, None] * THETA ** (-jnp.arange(half, dtype=F32) / half)
    cos, sin = jnp.cos(angle), jnp.sin(angle)
    return jnp.concatenate([cos, cos], 1), jnp.concatenate([-sin, sin], 1)


def _stacked(w):
    return w.reshape(w.shape[0], -1, TILE).transpose(1, 0, 2).reshape(-1, TILE)


def _unstacked(w):
    return w.reshape(-1, 64, TILE).transpose(1, 0, 2).reshape(64, -1)


def solution(mesh):
    def fetch(*parts):
        return lax.all_gather(parts[0] if len(parts) == 1 else jnp.concatenate(parts, 1), "dp", axis=0, tiled=True)

    def total(g):
        return lax.psum_scatter(g, "dp", scatter_dimension=0, tiled=True)

    def step(x, dy, wq, wk, wv, wo, wg, wu, wd):
        h0, dy = x[0], dy[0]
        d = h0.shape[1]
        cos, sin = rotary(h0.shape[0])
        qkv0 = fetch(wq[0], wk[0], wv[0])
        mid0 = fetch(wo[0], wg[0], wu[0])
        down0 = fetch(wd[0])
        attn1 = fetch(wq[1], wk[1], wv[1], wo[1])
        ffn1 = fetch(wd[1], _stacked(wg[1]), _stacked(wu[1]))
        wo0, wg0, wu0, wd0 = (mid0, 0), _columns(mid0, 1), _columns(mid0, 5), _down_of(down0)
        wo1, wg1, wu1, wd1 = (attn1, 3), _split(ffn1, 1), _split(ffn1, 2), _down_of(ffn1)

        a0, q0, k0, v0 = qkv(h0, qkv0, cos, sin)
        o0, lse0 = attend(q0, k0, v0)
        m0, b0 = attn_out(o0, h0, wo0)
        gu0, p0 = gate_up(b0, wg0, wu0)
        h1 = down(p0, m0, wd0)
        a1, q1, k1, v1 = qkv(h1, attn1, cos, sin)
        o1, lse1 = attend(q1, k1, v1)
        m1, b1 = attn_out(o1, h1, wo1)

        def first_half(dm, q, k, v, o, lse, a, h, w_o, w_qkv, f):
            do, delta = out_back(dm, w_o, o)
            dq, dk, dv = attend_back(q, k, v, do, lse, delta, cos, sin)
            g, dq, f = lax.optimization_barrier((attn_grads(a, dq, dk, dv, o, dm), dq, f))
            return total(g), qkv_back(dq, dk, dv, w_qkv, h, dm), f

        p1, dgu1 = ffn_last(b1, dy, wg1, wu1, wd1)
        g1, dgu1 = lax.optimization_barrier((ffn_grads(p1, dy, b1, dgu1), dgu1))
        f1 = total(g1.reshape(-1, 3 * TILE))
        dm1 = ffn_in(dgu1, wg1, wu1, m1, dy)
        t1, dh1, f1 = first_half(dm1, q1, k1, v1, o1, lse1, a1, h1, wo1, attn1, f1)
        dgu0 = ffn_back(dh1, wd0, gu0)
        g0, dgu0 = lax.optimization_barrier((ffn_grads(p0, dh1, b0, dgu0), dgu0))
        f0 = total(g0.reshape(-1, 3 * TILE))
        dm0 = ffn_in(dgu0, wg0, wu0, m0, dh1)
        dm0, t1 = lax.optimization_barrier((dm0, t1))
        t0, dx, f0 = first_half(dm0, q0, k0, v0, o0, lse0, a0, h0, wo0, qkv0, f0)

        attn = lambda n: jnp.stack([t[:, n * d : (n + 1) * d] for t in (t0, t1)])
        ffn = lambda n, form: jnp.stack([form(f[:, n * TILE : (n + 1) * TILE]) for f in (f0, f1)])
        return dx[None], attn(1), attn(2), attn(3), attn(0), ffn(1, _unstacked), ffn(2, _unstacked), ffn(0, lambda w: w)

    states, cut = P(("rep", "dp"), None, None), P(None, "dp", None)
    return jax.shard_map(
        step,
        mesh=mesh,
        in_specs=(states, states) + (cut,) * 7,
        out_specs=(states,) + (P("rep", "dp", None),) * 7,
        check_vma=False,
    )
```

```python
import functools

import jax
import jax.numpy as jnp
import numpy as np
from jax import lax
from jax.experimental import pallas as pl
from jax.experimental.pallas import tpu as pltpu
from jax.sharding import PartitionSpec as P

DEVICES = 16
HEAD = 128
HALF = HEAD // 2
THETA = 10000
NEG = -1e30
HIDDEN = 2 * NEG
LOG2E = 1.4426950408889634
SCALE = HEAD**-0.5
E = SCALE * LOG2E
VMEM = 64 * 2**20 - 2**16
TILE = 1024
WIDE = 512
PAIR = 2 * WIDE
BF16, F32 = jnp.bfloat16, jnp.float32
ANY = pl.BlockSpec(memory_space=pl.ANY)


def _dot(a, b, ca, cb):
    return lax.dot_general(a, b, (((ca,), (cb,)), ((), ())), preferred_element_type=F32)


def _nn(a, b):
    return _dot(a, b, 1, 0)


def _nt(a, b):
    return _dot(a, b, 1, 1)


def _tn(a, b):
    return _dot(a, b, 0, 0)


def _like(shape, dtype=BF16):
    return jax.ShapeDtypeStruct(shape, dtype)


def _call(kernel, grid, ins, outs, args, name, scratch=(), flops=0, **more):
    specs, shapes = zip(*outs)
    return pl.pallas_call(
        kernel,
        grid=grid,
        in_specs=list(ins),
        out_specs=list(specs),
        out_shape=list(shapes),
        scratch_shapes=list(scratch),
        compiler_params=pltpu.CompilerParams(dimension_semantics=("arbitrary",) * len(grid), vmem_limit_bytes=VMEM, **more),
        cost_estimate=pl.CostEstimate(flops=int(flops), bytes_accessed=int(flops) // TILE, transcendentals=0),
        name=name,
    )(*args)


def _rows(tile, cols):
    return pl.BlockSpec((tile, cols), lambda m, *_: (m, 0))


def _whole(shape, *at):
    at = at or (0,) * len(shape)
    return pl.BlockSpec(shape, lambda *_: at, pipeline_mode=pl.Buffered(1))


def _scale(wide):
    return lax.rsqrt(jnp.mean(wide * wide, -1, keepdims=True) + 1e-6)


def _normed(h):
    wide = h.astype(F32)
    return (wide * _scale(wide)).astype(BF16)


def _norm_back(h, g):
    wide, g = h.astype(F32), g.astype(F32)
    r = _scale(wide)
    return (g * r - wide * (r * r * r * jnp.mean(g * wide, -1, keepdims=True))).astype(BF16)


def _plus(a, b):
    return (a.astype(F32) + b.astype(F32)).astype(BF16)


def _flat(block):
    return block.reshape(-1, block.shape[-1])


def _columns(array):
    return array, lambda number, wide: pl.BlockSpec((array.shape[0], wide), lambda *ids: (0, number(*ids)))


def _split(view):
    def spec(number, wide):
        parts = 2 * PAIR // wide
        return pl.BlockSpec((DEVICES, 1, view.shape[2], wide), lambda *ids: (0, lax.div(number(*ids), parts), 0, lax.rem(number(*ids), parts)))

    return view, spec


def _down_of(array, at):
    return array, lambda number, high: pl.BlockSpec((high, TILE), lambda *ids: (number(*ids), at))


def _three(view, at):
    return view, _whole((DEVICES, 3, view.shape[2], TILE), 0, 0, 0, at)


def rotary(t):
    angle = np.arange(t, dtype=np.float32)[:, None] * np.float32(THETA) ** (-np.arange(HALF, dtype=np.float32) / np.float32(HALF))
    return jnp.asarray(np.concatenate([np.cos(angle), np.sin(angle)], -1))


def _angles(table):
    other = pltpu.roll(table, HALF, 1)
    first = lax.broadcasted_iota(jnp.int32, table.shape, 1) < HALF
    return jnp.where(first, table, other), jnp.where(first, -other, table)


def _qkv_kernel(h_ref, w_ref, table_ref, a_ref, *outs):
    cos, sin = _angles(table_ref[...])
    a = _normed(h_ref[...])
    a_ref[...] = a
    for n, out in enumerate(outs):
        t = _nn(a, _flat(w_ref[:, n])).astype(BF16)
        if n == 2:
            out[...] = t
            continue
        for at in range(0, TILE, HEAD):
            one = t[:, at : at + HEAD].astype(F32)
            out[:, at : at + HEAD] = (one * cos + pltpu.roll(one, HALF, 1) * sin).astype(BF16)


def qkv(h, w, table, tile=512):
    t, d = h.shape
    row = _rows(tile, d)
    return _call(_qkv_kernel, (t // tile,), [row, w[1], _rows(tile, HEAD)], [(row, _like((t, d)))] * 4, (h, w[0], table), "qkv",
                 flops=6 * t * d * d)


def _out_kernel(o_ref, h_ref, w_ref, h2_ref, b_ref):
    h2 = _plus(h_ref[...], _nn(o_ref[...], _flat(w_ref[...])).astype(BF16))
    h2_ref[...] = h2
    b_ref[...] = _normed(h2)


def attn_out(o, h, w, tile=512):
    t, d = h.shape
    row = _rows(tile, d)
    return _call(_out_kernel, (t // tile,), [row, row, w[1]], [(row, _like((t, d)))] * 2, (o, h, w[0]), "attn_out", flops=2 * t * d * d)


def _unit(g, u):
    s = 1 / (1 + jnp.exp(-g))
    silu = g * s
    return u * (s + silu * (1 - s)), silu


def _gate_up_kernel(b_ref, w_ref, by_ref, p_ref):
    w = _flat(w_ref[...])
    for n in range(2):
        y = _nn(b_ref[...], w[:, n * PAIR : (n + 1) * PAIR])
        u = y[:, WIDE:]
        by_g, by_u = _unit(y[:, :WIDE], u)
        at = n * PAIR
        by_ref[:, at : at + WIDE] = by_g
        by_ref[:, at + WIDE : at + PAIR] = by_u
        p_ref[:, n * WIDE : (n + 1) * WIDE] = (by_u * u).astype(BF16)


def gate_up(b, w, ff, tile=1024):
    t, d = b.shape
    return _call(_gate_up_kernel, (ff // PAIR, t // tile), [pl.BlockSpec((tile, d), lambda n, m: (m, 0)), w[1](lambda n, m: n, 2 * PAIR)],
                 [(pl.BlockSpec((tile, 2 * PAIR), lambda n, m: (m, n)), _like((t, 2 * ff), F32)), (pl.BlockSpec((tile, PAIR), lambda n, m: (m, n)), _like((t, ff)))],
                 (b, w[0]), "gate_up", flops=4 * t * d * ff)


def _long_kernel(x_ref, w_ref, *rest, back):
    *given, out_ref, acc = rest
    k = pl.program_id(1)

    @pl.when(k == 0)
    def _():
        acc[...] = jnp.zeros_like(acc)

    acc[...] += (_nt if back else _nn)(x_ref[...], _flat(w_ref[...]))

    @pl.when(k == pl.num_programs(1) - 1)
    def _():
        got = acc[...].astype(BF16)
        out_ref[...] = _plus(given[-1][...], _norm_back(given[0][...], got) if back else got)


def _long(x, w, given, back, deep, name, tile=1024):
    t, d = given[0].shape
    row = _rows(tile, d)
    return _call(functools.partial(_long_kernel, back=back), (t // tile, x.shape[1] // deep),
                 [pl.BlockSpec((tile, deep), lambda m, k: (m, k)), w[1](lambda m, k: k, deep), *[row] * len(given)], [(row, _like((t, d)))],
                 (x, w[0], *given), name, scratch=[pltpu.VMEM((tile, d), F32)], flops=2 * t * d * x.shape[1])[0]


def down(p, h, w):
    return _long(p, w, (h,), False, TILE, "down")


def ffn_in(dgu, w, h, dy):
    return _long(dgu, w, (h, dy), True, 2 * PAIR, "ffn_in")


def _ffn_all_kernel(b_ref, dy_ref, wd_ref, given_ref, *refs, last):
    p_ref, *refs = refs[-1:] + refs[:-1] if last else refs
    dgu_ref, out_hbm, down_s, up_s, sem = refs
    n = pl.program_id(0)
    steps = pl.num_programs(0)
    t, d = b_ref.shape

    def copies(n):
        slot = lax.rem(n, 2)
        rows, ff = down_s.shape[1:]
        yield pltpu.make_async_copy(down_s.at[slot], out_hbm.at[pl.ds(pl.multiple_of(n * rows, rows), rows), pl.ds(0, ff)], sem.at[slot, 0])
        yield pltpu.make_async_copy(up_s.at[slot], out_hbm.at[:, pl.ds(pl.multiple_of(ff + n * PAIR, PAIR), PAIR)], sem.at[slot, 1])

    @pl.when(n >= 2)
    def _():
        for one in copies(n - 2):
            one.wait()

    for at in range(0, t, TILE):
        rows = slice(at, at + TILE)
        dp = _nt(dy_ref[rows, :], wd_ref[...]).astype(BF16).astype(F32)
        if last:
            y = _nn(b_ref[rows, :], _flat(given_ref[...]))
            by_g, by_u = _unit(y[:, :WIDE], y[:, WIDE:])
            p_ref[rows, :] = (by_u * y[:, WIDE:]).astype(BF16)
        else:
            by_g, by_u = given_ref[rows, :WIDE], given_ref[rows, WIDE:]
        dgu_ref[rows, :WIDE] = (dp * by_g).astype(BF16)
        dgu_ref[rows, WIDE:] = (dp * by_u).astype(BF16)
    slot = lax.rem(n, 2)
    g = _tn(p_ref[...], dy_ref[...]).astype(BF16).reshape(-1, 4, d // DEVICES, d)
    for i in range(4):
        down_s[slot, :, i * d : (i + 1) * d] = _flat(g[:, i])
    up_s[slot] = _tn(b_ref[...], dgu_ref[...]).astype(BF16)
    for one in copies(n):
        one.start()

    @pl.when(n == steps - 1)
    def _():
        for at in (steps - 2, steps - 1):
            for one in copies(at):
                one.wait()


def ffn_all(b, dy, wd, ff, saved=None, w=None):
    t, d = dy.shape
    last = saved is None
    pair, one = (pl.BlockSpec((t, size), lambda n: (0, n)) for size in (PAIR, WIDE))
    number = lambda n: n
    more = [(w[0], w[1](number, PAIR))] if last else [(saved[0], pair), (saved[1], one)]
    return _call(functools.partial(_ffn_all_kernel, last=last), (ff // WIDE,), [_whole((t, d)), _whole((t, d)), wd[1](number, WIDE), *(s for _, s in more)],
                 [(pair, _like((t, 2 * ff))), (ANY, _like((d, 3 * ff)))], (b, dy, wd[0], *(a for a, _ in more)), "ffn_all",
                 scratch=[pltpu.VMEM((2, WIDE // 4, ff), BF16), pltpu.VMEM((2, d, PAIR), BF16), pltpu.SemaphoreType.DMA((2, 2)),
                          *([pltpu.VMEM((t, WIDE), BF16)] * last)],
                 flops=10 * t * d * ff)


def _out_back_kernel(dh_ref, w_ref, o_ref, do_ref, delta_ref):
    do = _nt(dh_ref[...], _flat(w_ref[...])).astype(BF16)
    do_ref[...] = do
    both = do.astype(F32) * o_ref[...].astype(F32)
    groups, heads, _ = delta_ref.shape
    for n in range(groups * heads):
        delta_ref[n // heads, n % heads, :] = both[:, n * HEAD : (n + 1) * HEAD].T.sum(axis=0)


def out_back(dh, w, o, stats, tile=512):
    t, d = dh.shape
    row = _rows(tile, d)
    return _call(_out_back_kernel, (t // tile,), [row, w[1], row], [(row, _like((t, d))), (pl.BlockSpec((*stats.shape[:2], tile), lambda m: (0, 0, m)), stats)],
                 (dh, w[0], o), "out_back", flops=2 * t * d * d)


def _over_keys(iq, bq, part):
    lax.fori_loop(0, iq, lambda j, _: part(pl.multiple_of(j * bq, bq), bq, 0, False), None)
    cut = bq // 2
    for first in (0, cut):
        part(pl.multiple_of(iq * bq + first, cut), cut, first, True)


def _mask(keys, queries):
    return lax.broadcasted_iota(jnp.int32, (keys, queries), 1) >= lax.broadcasted_iota(jnp.int32, (keys, queries), 0)


def _heads(ref):
    return [slice(at, at + HEAD) for at in range(0, ref.shape[1], HEAD)]


def _attend_kernel(q_ref, k_ref, v_ref, o_ref, lse_ref, top_s, mix_s):
    bq = q_ref.shape[0]
    heads = _heads(q_ref)
    top_s[...] = jnp.full_like(top_s, NEG)
    mix_s[...] = jnp.zeros_like(mix_s)

    def part(start, size, first, masked):
        here = pl.ds(start, size)
        ones = jnp.ones((8, size), BF16)
        ok = _mask(size, bq - first) if masked else None

        def score(i):
            return _nt(k_ref[here, heads[i]], q_ref[first:, heads[i]])

        def mix(i, p, keep):
            values = jnp.concatenate([v_ref[here, heads[i]].T, ones], axis=0)
            mix_s[i, :, first:] = mix_s[i, :, first:] * keep + _nn(values, p)

        ahead = 2
        scores, later = [score(i) for i in range(ahead)], None
        for i in range(len(heads)):
            if i + ahead < len(heads):
                scores.append(score(i + ahead))
            s = jnp.where(ok, scores[i], HIDDEN) if masked else scores[i]
            old = top_s[i, :, first:]
            top = jnp.maximum(old, s.max(axis=0, keepdims=True))
            top_s[i, :, first:] = top
            p, keep = jnp.exp2((s - top) * E).astype(BF16), jnp.exp2((old - top) * E)
            if later:
                mix(*later)
            later = i, p, keep
        mix(*later)

    _over_keys(pl.program_id(0), bq, part)
    for i, at in enumerate(heads):
        top, total = top_s[i], mix_s[i, HEAD : HEAD + 1, :]
        o_ref[:, at] = (mix_s[i, :HEAD, :] * (1 / total)).T.astype(BF16)
        group = lse_ref.shape[1]
        lse_ref[i // group, i % group : i % group + 1, :] = top * SCALE + jnp.log(total)


def attend(q, k, v, stats, bq=512):
    t, d = q.shape
    heads = d // HEAD
    row = _rows(bq, d)
    return _call(_attend_kernel, (t // bq,), [row, _whole((t, d)), _whole((t, d))],
                 [(row, _like((t, d))), (pl.BlockSpec((*stats.shape[:2], bq), lambda m: (0, 0, m)), stats)], (q, k, v), "attend",
                 scratch=[pltpu.VMEM((heads, 1, bq), F32), pltpu.VMEM((heads, HEAD + 8, bq), F32)], flops=4 * t * t * d)


def _attend_back_kernel(q_ref, k_ref, v_ref, do_ref, lse_ref, delta_ref, table_ref, dq_ref, dk_ref, dv_ref, dq_s, dk_s, dv_s):
    iq = pl.program_id(1)
    bq = q_ref.shape[0]
    heads = _heads(q_ref)

    @pl.when(iq == 0)
    def _():
        dk_s[...] = jnp.zeros_like(dk_s)
        dv_s[...] = jnp.zeros_like(dv_s)

    dq_s[...] = jnp.zeros_like(dq_s)
    lses = [lse_ref[0, i : i + 1, :] * LOG2E for i in range(len(heads))]
    deltas = [delta_ref[0, i : i + 1, :] for i in range(len(heads))]

    def part(start, size, first, masked):
        here = pl.ds(start, size)
        ok = _mask(size, bq - first) if masked else None
        scores = [_nt(k_ref[here, at], q_ref[first:, at]) for at in heads]
        dps = [_nt(v_ref[here, at], do_ref[first:, at]) for at in heads]
        for i, at in enumerate(heads):
            p = jnp.exp2(scores[i] * E - lses[i][:, first:])
            if masked:
                p = jnp.where(ok, p, 0.0)
            ds = (p * (dps[i] - deltas[i][:, first:])).astype(BF16)
            dv_s[here, at] += _nn(p.astype(BF16), do_ref[first:, at])
            dk_s[here, at] += _nn(ds, q_ref[first:, at])
            dq_s[i, :, first:] += _nn(k_ref[here, at].T, ds)

    def turned_back(g, table):
        cos, sin = _angles(table)
        g = g.astype(BF16).astype(F32)
        return (g * cos + pltpu.roll(g * sin, HALF, 1)).astype(BF16)

    _over_keys(iq, bq, part)
    for i, at in enumerate(heads):
        dq_ref[:, at] = turned_back((dq_s[i] * SCALE).T, table_ref[pl.ds(pl.multiple_of(iq * bq, bq), bq), :])

    @pl.when(iq == pl.num_programs(1) - 1)
    def _():
        for at in heads:
            dk_ref[:, at] = turned_back(dk_s[:, at] * SCALE, table_ref[...])
        dv_ref[...] = dv_s[...].astype(BF16)


def attend_back(q, k, v, do, lse, delta, table, bq=512):
    t, d = q.shape
    group = lse.shape[1]
    w = group * HEAD
    row = pl.BlockSpec((bq, w), lambda ih, iq: (iq, ih))
    keys = pl.BlockSpec((t, w), lambda ih, iq: (0, ih))
    stats = pl.BlockSpec((1, group, bq), lambda ih, iq: (ih, 0, iq))
    one = _like((t, d))
    return _call(_attend_back_kernel, (d // w, t // bq), [row, keys, keys, row, stats, stats, _whole(table.shape)], [(row, one), (keys, one), (keys, one)],
                 (q, k, v, do, lse, delta, table), "attend_back",
                 scratch=[pltpu.VMEM((group, HEAD, bq), F32), *[pltpu.VMEM((t, w), F32)] * 2], flops=10 * t * t * d)


COLOURS = (((0, 384), "xyz"), ((384, 768), "yzx"), ((768, 1024), "zxy"))
MESH = pl.DeviceIdType.MESH
PLACE = {"x": 8, "y": 4, "z": 2, "core": 1}


def _here():
    me = lax.axis_index("dp")
    return me, {axis: lax.rem(lax.div(me, weight), 2) for axis, weight in PLACE.items()}


def _across(me, axis):
    weight = PLACE[axis]
    return {"dp": me + weight - 2 * weight * lax.rem(lax.div(me, weight), 2)}


def _send(me, axis, src, dst, send, recv):
    return pltpu.make_async_remote_copy(src_ref=src, dst_ref=dst, send_sem=send, recv_sem=recv, device_id=_across(me, axis), device_id_type=MESH)


def _greet(me):
    barrier = pltpu.get_barrier_semaphore()
    for axis in PLACE:
        pl.semaphore_signal(barrier, inc=1, device_id=_across(me, axis), device_id_type=MESH)
    pl.semaphore_wait(barrier, len(PLACE))


def _blocks(bits, order, n, flip):
    index = [slice(None)] * 3
    for i, axis in enumerate(order[:n]):
        index["xyz".index(axis)] = 1 - bits[axis] if flip and i + 1 == n else bits[axis]
    return tuple(index)


def _first_half_kernel(o_hbm, dm_hbm, a_hbm, dq_hbm, dk_hbm, dv_hbm, w_hbm, h_ref, dx_ref, grad_ref, left, right, total, *rest):
    outs, ins, (load, send0, recv0, send, recv) = rest[:4], rest[4:8], rest[8:]
    step = pl.program_id(0)
    me, bits = _here()
    core = bits["core"]
    t, d = dm_hbm.shape
    part = d // DEVICES
    matrices = right.shape[0]
    lines = lambda at, size: pl.ds(pl.multiple_of(lax.div(at, part), DEVICES), size // part)
    loads = [pltpu.make_async_copy(src, dst, load.at[n]) for n, (src, dst) in enumerate((
        (o_hbm, left.at[lines(t, t)]), (dm_hbm, right.at[0]), (a_hbm, left.at[lines(0, t)]), (dq_hbm, right.at[1]), (dk_hbm, right.at[2]),
        (dv_hbm, right.at[3]), *((w_hbm.at[:, n, :, pl.ds(w_hbm.shape[3] - d, d)], left.at[lines(t + n * d, d)]) for n in range(3))))]
    first, after = loads[:6], loads[6:]

    def core_copy(m):
        return _send(me, "core", outs[0].at[m], ins[0].at[m], send0.at[m], recv0.at[m])

    def chip_copies(m, n):
        for colour, ((start, stop), order) in enumerate(COLOURS):
            at = (m, *[slice(None)] * (4 - n), slice(start, stop))
            yield _send(me, order[n - 1], outs[n].at[at], ins[n].at[at], send.at[m, n - 1, colour], recv.at[m, n - 1, colour])

    def pass_on(m, n):
        for (start, stop), order in COLOURS:
            cols = slice(start, stop)
            outs[n][(m, *[slice(None)] * (4 - n), cols)] = total[(m, *_blocks(bits, order, n, True), slice(None), cols)].astype(BF16)
        for one in chip_copies(m, n):
            one.start()

    @pl.when(step == 0)
    def _():
        for one in first:
            one.start()
        _greet(me)
        for one in first[:2]:
            one.wait()

    @pl.when(step == 1)
    def _():
        for one in after:
            one.start()
        for one in first[2:4]:
            one.wait()

    for n in (2, 3):

        @pl.when(step == n)
        def _():
            first[n + 2].wait()

    @pl.when(step < matrices)
    def _():
        start = pl.multiple_of(jnp.where(step == 0, t, 0), t)

        def columns(n, _):
            cols = pl.ds(pl.multiple_of(n * WIDE, WIDE), WIDE)
            g = _tn(_flat(left[lines(start, t)]), right[step, :, cols]).reshape(2, 2, 2, 2, part, WIDE)
            even, odd = g[:, :, :, 0], g[:, :, :, 1]
            total[step, :, :, :, :, cols] = jnp.where(core == 0, even, odd)
            outs[0][step, :, :, :, :, cols] = jnp.where(core == 0, odd, even).astype(BF16)

        lax.fori_loop(0, d // WIDE, columns, None)

    @pl.when(step == matrices)
    def _():
        for one in after:
            one.wait()

    @pl.when(step >= matrices)
    def _():
        rows = pl.ds(pl.multiple_of((step - matrices) * h_ref.shape[0], h_ref.shape[0]), h_ref.shape[0])
        acc = sum(_nt(right[1 + n, rows, :], _flat(left[lines(t + n * d, d)])) for n in range(3))
        dx_ref[...] = _plus(right[0, rows, :], _norm_back(h_ref[...], acc.astype(BF16)))

    for n in (3, 2, 1):
        m = step - n - 1

        @pl.when((m >= 0) & (m < matrices))
        def _():
            for one, ((start, stop), order) in zip(chip_copies(m, n), COLOURS):
                one.wait()
                cols = slice(start, stop)
                keep = (m, *_blocks(bits, order, n, False), slice(None), cols)
                value = total[keep] + ins[n][(m, *[slice(None)] * (4 - n), cols)].astype(F32)
                if n == 3:
                    grad_ref[:, pl.ds(pl.multiple_of(m * d + start, HEAD), stop - start)] = value.astype(BF16)
                else:
                    total[keep] = value
            if n < 3:
                pass_on(m, n + 1)

    @pl.when((step >= 1) & (step <= matrices))
    def _():
        m = step - 1
        core_copy(m).wait()
        total[m] = total[m] + ins[0][m].astype(F32)
        pass_on(m, 1)

    @pl.when(step < matrices)
    def _():
        core_copy(step).start()


def first_half_grads(layer, o, dm, a, dq, dk, dv, w, h, tile=512):
    t, d = h.shape
    part = d // DEVICES
    rows = pl.BlockSpec((tile, d), lambda s: (jnp.maximum(s - 4, 0), 0))
    blocks = lambda n: (4, *[2] * n, part, d)
    sems = pltpu.SemaphoreType.DMA
    return _call(_first_half_kernel, (8,), [ANY] * 7 + [rows], [(rows, _like((t, d))), (pl.BlockSpec((part, 4 * d), lambda s: (0, 0)), _like((part, 4 * d)))],
                 (o.reshape(-1, part, d), dm, a.reshape(-1, part, d), dq, dk, dv, w, h), "first_half_grads",
                 scratch=[pltpu.VMEM(((t + 3 * d) // part, part, d), BF16), pltpu.VMEM((4, t, d), BF16), pltpu.VMEM(blocks(3), F32),
                          *[pltpu.VMEM(blocks(n), BF16) for n in (3, 2, 1, 0)] * 2, sems((9,)), sems((4,)), sems((4,)), sems((4, 3, 3)), sems((4, 3, 3))],
                 flops=14 * t * d * d, collective_id=layer, has_side_effects=True)


def _fetch_kernel(*refs):
    *given, out, load, send, recv, send0, recv0 = refs
    me, bits = _here()
    core = bits["core"]
    orders = [order for _, order in COLOURS]
    chip = tuple(bits[axis] for axis in "xyz")
    loads = [pltpu.make_async_copy(src.at[0], out.at[(*chip, core, m)], load.at[m]) for m, src in enumerate(given)]
    for one in loads:
        one.start()

    def have(n, order, flip):
        index = list(chip)
        for i, axis in enumerate(order[:n]):
            index["xyz".index(axis)] = 1 - bits[axis] if flip and i + 1 == n else slice(None)
        return tuple(index)

    def chip_copy(n, m):
        at = out.at[(*have(n, orders[m], False), core, m)]
        return _send(me, orders[m][n], at, at, send.at[n, m], recv.at[n, m])

    def core_copy(n, m):
        at = out.at[(*have(n, orders[m], n > 0), core, m)]
        return _send(me, "core", at, at, send0.at[n, m], recv0.at[n, m])

    _greet(me)
    for n in range(4):
        for m, one in enumerate(loads):
            if n == 0:
                one.wait()
            else:
                chip_copy(n - 1, m).wait_recv()
            if n < 3:
                chip_copy(n, m).start()
        for m in range(3):
            core_copy(n, m).start()
    for n in range(4):
        for m in range(3):
            core_copy(n, m).wait()
            if n < 3:
                chip_copy(n, m).wait_send()


def fetch_first(*given):
    _, rows, d = given[0].shape
    shape = (*[2] * 4, 3, rows, d)
    sems = pltpu.SemaphoreType.DMA
    out = _call(_fetch_kernel, (1,), [ANY] * 3, [(_whole(shape), _like(shape))], given, "fetch_first",
                scratch=[sems((3,)), sems((3, 3)), sems((3, 3)), sems((4, 3)), sems((4, 3))], flops=10**10, collective_id=2, has_side_effects=True)
    return out[0].reshape(DEVICES, 3, rows, d)


def _move_kernel(*refs, moves, ins):
    given, outs, sem = refs[:ins], refs[ins:-1], refs[-1]
    copies = [pltpu.make_async_copy(given[i].at[src], outs[o].at[dst], sem.at[n]) for n, (i, src, o, dst) in enumerate(moves)]
    for one in copies:
        one.start()
    for one in copies:
        one.wait()


def move(given, moves, shapes, name):
    return _call(functools.partial(_move_kernel, moves=moves, ins=len(given)), (1,), [_whole(*block) for _, *block in given], [(ANY, _like(s)) for s in shapes],
                 [a for a, *_ in given], name, scratch=[pltpu.SemaphoreType.DMA((len(moves),))])


def _cut(n, size, start=0):
    return slice(start + n * size, start + (n + 1) * size)


def solution(mesh):
    def fetch(shard):
        return lax.all_gather(shard, "dp", axis=0, tiled=True)

    def total(g):
        return lax.psum_scatter(g, "dp", scatter_dimension=0, tiled=True)

    def step(x, dy, wq, wk, wv, wo, wg, wu, wd):
        h0, dy = x[0], dy[0]
        t, d = h0.shape
        r, ff = wq.shape[1], wg.shape[2]
        groups = range(ff // WIDE)
        table = rotary(t)
        stats = _like((2, d // HEAD // 2, t), F32)
        of = lambda w, layer: (w, (1, *w.shape[1:]), layer, 0, 0)
        lines = lambda n: (0, _cut(n, r))
        view = lambda w: w.reshape(DEVICES, -1, r, w.shape[-1])

        moves = [(i, (0, slice(None), _cut(n, WIDE)), 0, (slice(None), _cut(2 * n + i, WIDE))) for n in groups for i in (0, 1)]
        moves += [(2, (0,), 0, (slice(None), _cut(0, d, 2 * ff)))]
        shard, wq = lax.optimization_barrier((*move((of(wg, 0), of(wu, 0), of(wo, 0)), moves, [(r, 2 * ff + d)], "pack"), wq))
        mid0 = fetch(shard)
        qkv0 = fetch_first(wq, wk, wv)
        a0, q0, k0, v0 = qkv(h0, _three(qkv0, 0), table)
        a0, wq, wk, wv, wo, wg, wu, wd = lax.optimization_barrier((a0, wq, wk, wv, wo, wg, wu, wd))
        moves = [(0, (0,), 0, (slice(None), _cut(0, d)))] + [(n + 1, (0,), 0, (_cut(n, r), _cut(1, d))) for n in range(4)]
        next1 = fetch(*move((of(wd, 0), *(of(w, 1) for w in (wq, wk, wv, wo))), moves, [(4 * r, 2 * d)], "pack"))
        moves = [(i, (0, slice(None), _cut(n, WIDE)), 0, (_cut(n // 2, r), _cut(n % 2 * 2 + i, WIDE))) for n in groups for i in (0, 1)]
        moves += [(2, (0,), 0, (slice(None), _cut(2, d)))]
        ffn1 = fetch(*move((of(wg, 1), of(wu, 1), of(wd, 1)), moves, [(4 * r, 3 * d)], "pack"))
        attn1 = view(next1)
        wo0, wgu0, wd0 = (mid0, _whole((d, d), 0, 2 * ff // d)), _columns(mid0), _down_of(next1, 0)
        wo1, wgu1, wd1 = (attn1, _whole((DEVICES, 1, r, d), 0, 3, 0, 1)), _split(view(ffn1)), _down_of(ffn1, 2)
        o0, lse0 = attend(q0, k0, v0, stats)
        m0, b0 = attn_out(o0, h0, wo0)
        saved = gate_up(b0, wgu0, ff)
        h1 = down(saved[1], m0, wd0)
        a1, q1, k1, v1 = qkv(h1, _three(attn1, 1), table)
        o1, lse1 = attend(q1, k1, v1, stats)
        m1, b1 = attn_out(o1, h1, wo1)

        def first_half(layer, dm, q, k, v, o, lse, a, h, w_o, w_qkv):
            do, delta = out_back(dm, w_o, o, stats)
            dq, dk, dv = attend_back(q, k, v, do, lse, delta, table)
            return first_half_grads(layer, o, dm, a, dq, dk, dv, w_qkv, h)

        dgu, g = lax.optimization_barrier(ffn_all(b1, dy, wd1, ff, w=wgu1))
        f1 = total(g)
        dh1, t1 = first_half(1, ffn_in(dgu, wgu1, m1, dy), q1, k1, v1, o1, lse1, a1, h1, wo1, attn1)
        dh1, f1 = lax.optimization_barrier((dh1, f1))
        dgu, g = lax.optimization_barrier(ffn_all(b0, dh1, wd0, ff, saved=saved))
        f0 = total(g)
        dx, t0 = first_half(0, ffn_in(dgu, wgu0, m0, dh1), q0, k0, v0, o0, lse0, a0, h0, wo0, qkv0)

        moves = []
        for layer in (0, 1):
            moves += [(2 + layer, (slice(None), _cut((n + 1) % 4, d)), n, (layer,)) for n in range(4)]
            moves += [(layer, (slice(None), _cut(2 * n + i, WIDE, ff)), 4 + i, (layer, slice(None), _cut(n, WIDE))) for n in groups for i in (0, 1)]
            moves += [(layer, (slice(None), _cut(n, d)), 6, (layer, _cut(n, r))) for n in range(4)]
        moves += [(4, (), 7, (0,))]
        shapes = [(2, r, d)] * 4 + [(2, r, ff)] * 2 + [(2, 4 * r, d), (1, t, d)]
        *grads, dx = move([(a, a.shape) for a in (f0, f1, t0, t1, dx)], moves, shapes, "results")
        return dx, *grads

    states, cut = P(("rep", "dp"), None, None), P(None, "dp", None)
    return jax.shard_map(
        step,
        mesh=mesh,
        in_specs=(states, states) + (cut,) * 7,
        out_specs=(states,) + (P("rep", "dp", None),) * 7,
        check_vma=False,
    )
```
